32 devices in a mesh: batch: 4 (over x, core), seq: 8 (over z, y).
Axes of the slice: x: 2, y: 2, z: 4, core: 2. Of those that a mesh axis runs over, the one named last changes fastest.
Arguments:
- signal: bfloat16 [4, 2048, 256], P('batch', 'seq'), may hold values from -0.3125 to 0.3125
- grad_out: bfloat16 [4, 2048, 256], P('batch', 'seq'), may hold values from -6 to 6
- filter_taps: float32 [2048, 256], P('seq'), may hold values from -0.3125 to 0.3125
- skip_gain: float32 [256], replicated, may hold values from 0.5 to 2
Outputs:
- input_grad: bfloat16 [4, 2048, 256], P('batch', 'seq')
- filter_grad: float32 [2048, 256], P('seq')
The draws below stay inside these ranges and needn't reach their ends.
All inputs are finite; a program needn't handle non-finite values.
Results may differ from the reference program's by a relative error of at most 0.001.
Values sent between devices are 32-bit elements; how exact they have to be, the bound alone decides.
A program may use at most 64 MiB of HBM per device.

```python
import jax
import jax.numpy as jnp

CHANNELS = 256
LENGTH = 2048
BATCH = 4


def levels(stream_key, dims, pieces, least, high):
    factor_of, own = 1.0, jax.random.fold_in(stream_key, 6)
    for dim, blocks in pieces:
        heights = jnp.exp(jax.random.uniform(jax.random.fold_in(own, dim), (blocks,), jnp.float32, least / len(pieces), high / len(pieces)))
        factor_of = factor_of * jnp.repeat(heights, dims[dim] // blocks).reshape([-1 if axis == dim else 1 for axis in range(len(dims))])
    return factor_of


def scatter_about(own_key, dims, width, bound, shards=(), dtype=jnp.bfloat16):
    array = width * jax.random.normal(own_key, dims, jnp.float32)
    if shards:
        array = array * levels(own_key, dims, shards, -0.22, 0.18)
    return jnp.clip(array, -bound, bound).astype(dtype)


def setup_inputs(seed: int = 0) -> dict:
    keys = jax.random.split(jax.random.key(seed), 5)
    return {
        "signal": scatter_about(keys[0], (BATCH, LENGTH, CHANNELS), (LENGTH ** -0.5), 0.3125, ((0, 4), (1, 8))),
        "grad_out": scatter_about(keys[1], (BATCH, LENGTH, CHANNELS), 1.0, 6.0, ((0, 4), (1, 8))),
        "filter_taps": scatter_about(keys[2], (LENGTH, CHANNELS), (LENGTH ** -0.5), 0.3125, ((0, 8),), jnp.float32),
        "skip_gain": jnp.clip(jax.random.uniform(keys[3], (CHANNELS,), jnp.float32, 0.5, 2.0), 0.5, 2.0),
    }


def reference(signal, grad_out, filter_taps, skip_gain):
    length = signal.shape[1]
    padded_len = 2 * length
    signal_full = signal.astype(jnp.float32)
    grad_full = grad_out.astype(jnp.float32)
    signal_spec = jnp.fft.rfft(signal_full, n=padded_len, axis=1)
    grad_spec = jnp.fft.rfft(grad_full, n=padded_len, axis=1)
    taps_spec = jnp.fft.rfft(filter_taps, n=padded_len, axis=0)
    input_conv = jnp.fft.irfft(grad_spec * jnp.conj(taps_spec)[None], n=padded_len, axis=1)[:, :length]
    input_grad = (input_conv + skip_gain[None, None, :] * grad_full).astype(jnp.bfloat16)
    summed = jnp.sum(grad_spec * jnp.conj(signal_spec), axis=0)
    filter_grad = jnp.fft.irfft(summed, n=padded_len, axis=0)[:length]
    return input_grad, filter_grad.astype(jnp.float32)
```

```python
import functools
import math

import jax
import jax.numpy as jnp
import numpy as np
from jax import lax
from jax.experimental import pallas as pl
from jax.experimental.pallas import tpu as pltpu
from jax.sharding import PartitionSpec as P

MESH = pl.DeviceIdType.MESH
F32 = jnp.float32
BF16 = jnp.bfloat16
GRAD, TAPS, SIGNAL, INPUT, FILTER = range(5)


def weighted(terms):
    total = None
    for factor, array in terms:
        if array is None or abs(factor) < 1e-12:
            continue
        if total is None:
            if abs(factor - 1.0) < 1e-12:
                total = array
            else:
                total = array * factor
        elif abs(factor - 1.0) < 1e-12:
            total = total + array
        elif abs(factor + 1.0) < 1e-12:
            total = total - array
        else:
            total = total + array * factor
    return total


def added(left, right):
    return weighted([(1.0, left), (1.0, right)])


def subtracted(left, right):
    return weighted([(1.0, left), (-1.0, right)])


def turn(real, imag, cos_turn, sin_turn):
    if imag is None:
        return real * cos_turn, -(real * sin_turn)
    return real * cos_turn + imag * sin_turn, imag * cos_turn - real * sin_turn


def coarse_forward(blocks):
    count = len(blocks)
    result = [None] * (count + 1)
    for k in range(count // 2 + 1):
        sums = []
        for parity in (0, 1):
            angles = [(math.pi * ((s * k) % (2 * count)) / count, s) for s in range(parity, count, 2)]
            sums.append(
                (
                    weighted([(math.cos(a), blocks[s]) for a, s in angles]),
                    weighted([(-math.sin(a), blocks[s]) for a, s in angles]),
                )
            )
        (even_re, even_im), (odd_re, odd_im) = sums
        result[k] = (added(even_re, odd_re), added(even_im, odd_im))
        if k != count - k:
            result[count - k] = (subtracted(even_re, odd_re), subtracted(odd_im, even_im))
    return result


def coarse_inverse(terms, scale):
    count = len(terms) - 1
    pairs = []
    for k in range(count // 2 + 1):
        weight = scale if k == 0 else 2.0 * scale
        real, imag = terms[k]
        if k == count - k:
            pairs.append((weight, real, imag, real, imag))
        else:
            other_re, other_im = terms[count - k]
            pairs.append((weight, real + other_re, imag - other_im, real - other_re, imag + other_im))
    blocks = []
    for s in range(count):
        parts = []
        for k, (weight, even_re, even_im, odd_re, odd_im) in enumerate(pairs):
            angle = math.pi * ((s * k) % (2 * count)) / count
            parts.append((weight * math.cos(angle) * (1 if abs(math.cos(angle)) > 1e-9 else 0), odd_re if s % 2 else even_re))
            parts.append((weight * math.sin(angle) * (1 if abs(math.sin(angle)) > 1e-9 else 0), odd_im if s % 2 else even_im))
        blocks.append(weighted(parts))
    return blocks


def fused_kernel(
    groups, seqs,
    signal_ref, grad_ref, tap_ref, skip_ref, high_ref, low_ref, cos_ref, sin_ref,
    input_ref, filter_ref,
    grad_out_buf, signal_out_buf, tap_out_buf, grad_in, signal_in, tap_in,
    input_out, filter_out, input_in, filter_in,
    grad_rows, grad_spec, signal_rows, signal_spec, input_rows, filter_rows, filter_spec,
    send_sems, recv_sems,
):
    count = groups * seqs
    coarse = seqs + 1
    own, rows = grad_in.shape[1:]
    channels = count * own
    group, seq = lax.axis_index("batch"), lax.axis_index("seq")
    me = group * seqs + seq
    scale = 1.0 / (2 * seqs * rows)
    re, im = pl.ds(0, rows), pl.ds(rows, rows)

    def peer(step):
        place = lax.rem(me + step, count)
        return place, lax.div(place, seqs), lax.rem(place, seqs)

    barrier = pltpu.get_barrier_semaphore()

    def greet(step, carry):
        _, to_group, to_seq = peer(step)
        pl.semaphore_signal(
            barrier, inc=1, device_id={"batch": to_group, "seq": to_seq}, device_id_type=MESH
        )
        return carry

    lax.fori_loop(1, count, greet, 0)

    def transfer(source, target, kind, to_group, to_seq):
        return pltpu.make_async_remote_copy(
            src_ref=source,
            dst_ref=target,
            send_sem=send_sems.at[kind],
            recv_sem=recv_sems.at[kind],
            device_id={"batch": to_group, "seq": to_seq},
            device_id_type=MESH,
        )

    def all_of(buffer, blocks, kind):
        _, to_group, to_seq = peer(1)
        view = buffer.at[pl.ds(0, blocks)]
        return transfer(view, view, kind, to_group, to_seq)

    grad_out_buf[...] = grad_ref[...].astype(F32).T.reshape(count, own, rows)
    tap_out_buf[...] = tap_ref[...].T.reshape(count, own, rows)
    signal_out_buf[...] = signal_ref[...].astype(F32).T.reshape(count, own, rows)
    pl.semaphore_wait(barrier, count - 1)

    def send_taps(step, carry):
        to_seq = lax.rem(seq + step, seqs)
        place = group * seqs + to_seq
        transfer(tap_out_buf.at[place], tap_in.at[seq], TAPS, group, to_seq).start()
        return carry

    def send_grads(step, carry):
        place, to_group, to_seq = peer(step)
        transfer(grad_out_buf.at[place], grad_in.at[me], GRAD, to_group, to_seq).start()
        return carry

    def send_signals(step, carry):
        place, to_group, to_seq = peer(step)
        transfer(signal_out_buf.at[place], signal_in.at[me], SIGNAL, to_group, to_seq).start()
        return carry

    lax.fori_loop(1, seqs, send_taps, 0)
    lax.fori_loop(1, count, send_grads, 0)
    lax.fori_loop(1, count, send_signals, 0)
    grad_in[me] = grad_out_buf[me]
    tap_in[seq] = tap_out_buf[me]
    signal_in[me] = signal_out_buf[me]

    def spread(blocks, target, first_row):
        place = pl.ds(first_row, own)
        for k, (real, imag) in enumerate(coarse_forward(blocks)):
            real, imag = turn(real, imag, cos_ref[k], sin_ref[k])
            target[k, place, re] = real
            target[k, place, im] = imag

    def fine(source, target):
        lines = source.shape[0] * source.shape[1]
        value = source[...].reshape(lines, 2 * rows)
        high = value.astype(BF16)
        low = (value - high.astype(F32)).astype(BF16)
        product = functools.partial(jnp.dot, preferred_element_type=F32)
        total = product(high, high_ref[...]) + product(low, high_ref[...]) + product(high, low_ref[...])
        target[...] = total.reshape(target.shape)

    def collect(source, first_row):
        place = pl.ds(first_row, own)
        terms = [
            turn(source[k, place, re], source[k, place, im], cos_ref[k], sin_ref[k])
            for k in range(coarse)
        ]
        return coarse_inverse(terms, scale)

    def row_of(index):
        return pl.multiple_of(index * own, own)

    all_of(tap_in, seqs - 1, TAPS).wait_recv()
    spread([tap_in[s] for s in range(seqs)], grad_rows, groups * own)
    all_of(grad_in, count - 1, GRAD).wait_recv()

    def spread_grad(index, carry):
        spread([grad_in[index * seqs + s] for s in range(seqs)], grad_rows, row_of(index))
        return carry

    lax.fori_loop(0, groups, spread_grad, 0)
    fine(grad_rows, grad_spec)

    def multiply_taps(index, carry):
        place, fixed = pl.ds(row_of(index), own), pl.ds(groups * own, own)
        for k in range(coarse):
            grad_re, grad_im = grad_spec[k, place, re], grad_spec[k, place, im]
            tap_re, tap_im = grad_spec[k, fixed, re], grad_spec[k, fixed, im]
            input_rows[k, place, re] = grad_re * tap_re + grad_im * tap_im
            input_rows[k, place, im] = grad_re * tap_im - grad_im * tap_re
        return carry

    lax.fori_loop(0, groups, multiply_taps, 0)
    fine(input_rows, input_rows)

    def collect_input(index, carry):
        for s, block in enumerate(collect(input_rows, row_of(index))):
            input_out[index * seqs + s] = block
        return carry

    lax.fori_loop(0, groups, collect_input, 0)

    def send_inputs(step, carry):
        place, to_group, to_seq = peer(step)
        transfer(input_out.at[place], input_in.at[me], INPUT, to_group, to_seq).start()
        return carry

    lax.fori_loop(1, count, send_inputs, 0)
    input_in[me] = input_out[me]

    all_of(signal_in, count - 1, SIGNAL).wait_recv()

    def spread_signal(index, carry):
        spread([signal_in[index * seqs + s] for s in range(seqs)], signal_rows, row_of(index))
        return carry

    lax.fori_loop(0, groups, spread_signal, 0)
    fine(signal_rows, signal_spec)
    for k in range(coarse):
        real, imag = None, None
        for index in range(groups):
            place = pl.ds(index * own, own)
            grad_re, grad_im = grad_spec[k, place, re], grad_spec[k, place, im]
            signal_re, signal_im = signal_spec[k, place, re], signal_spec[k, place, im]
            real = added(real, grad_re * signal_re + grad_im * signal_im)
            imag = added(imag, grad_re * signal_im - grad_im * signal_re)
        filter_rows[k, :, re] = real
        filter_rows[k, :, im] = imag
    fine(filter_rows, filter_spec)
    for s, block in enumerate(collect(filter_spec, 0)):
        filter_out[s] = block

    def send_filters(step, carry):
        _, to_group, to_seq = peer(step)
        transfer(filter_out.at[to_seq], filter_in.at[me], FILTER, to_group, to_seq).start()
        return carry

    lax.fori_loop(1, count, send_filters, 0)
    filter_in[me] = filter_out[seq]

    all_of(input_in, count - 1, INPUT).wait_recv()
    gradient = input_in[...].reshape(channels, rows).T + skip_ref[...] * grad_ref[...].astype(F32)
    input_ref[...] = gradient.astype(BF16)
    all_of(filter_in, count - 1, FILTER).wait_recv()
    filter_ref[...] = filter_in[...].reshape(channels, rows).T
    for kind, buffer in ((GRAD, grad_in), (SIGNAL, signal_in), (INPUT, input_in), (FILTER, filter_in)):
        all_of(buffer, count - 1, kind).wait_send()
    all_of(tap_in, seqs - 1, TAPS).wait_send()


def fine_tables(rows):
    grid = np.arange(rows)
    angle = 2.0 * np.pi / rows * (np.outer(grid, grid) % rows)
    table = np.block([[np.cos(angle), -np.sin(angle)], [np.sin(angle), np.cos(angle)]]).astype(np.float32)
    high = table.astype(BF16)
    return high, (table - high.astype(np.float32)).astype(BF16)


def turn_tables(seqs, rows, lines):
    angle = np.pi / (seqs * rows) * np.outer(np.arange(seqs + 1), np.arange(rows))
    wide = np.broadcast_to(angle[:, None, :], (seqs + 1, lines, rows))
    return np.cos(wide).astype(np.float32), np.sin(wide).astype(np.float32)


def fused_shards(groups, seqs, signal, grad_out, filter_taps, skip_gain):
    rows, channels = filter_taps.shape
    count, coarse = groups * seqs, seqs + 1
    own = channels // count
    high, low = fine_tables(rows)
    cos_turn, sin_turn = turn_tables(seqs, rows, own)
    blocks = pltpu.VMEM((count, own, rows), F32)
    few = pltpu.VMEM((seqs, own, rows), F32)
    lines = lambda number: pltpu.VMEM((coarse, number * own, 2 * rows), F32)
    vmem = pl.BlockSpec(memory_space=pltpu.VMEM)
    input_grad, filter_grad = pl.pallas_call(
        functools.partial(fused_kernel, groups, seqs),
        out_shape=(
            jax.ShapeDtypeStruct((rows, channels), BF16),
            jax.ShapeDtypeStruct((rows, channels), F32),
        ),
        in_specs=[vmem] * 8,
        out_specs=(vmem, vmem),
        scratch_shapes=[
            blocks, blocks, blocks, blocks, blocks, few,
            blocks, few, blocks, blocks,
            lines(groups + 1), lines(groups + 1), lines(groups), lines(groups),
            lines(groups), lines(1), lines(1),
            pltpu.SemaphoreType.DMA((5,)),
            pltpu.SemaphoreType.DMA((5,)),
        ],
        compiler_params=pltpu.CompilerParams(
            collective_id=0, has_side_effects=True, vmem_limit_bytes=48 * 1024 * 1024
        ),
    )(
        signal[0], grad_out[0], filter_taps, skip_gain[None, :],
        jnp.asarray(high), jnp.asarray(low), jnp.asarray(cos_turn), jnp.asarray(sin_turn),
    )
    return input_grad[None], filter_grad


def fits_fused(groups, seqs, signal, filter_taps):
    rows, channels = filter_taps.shape
    return (
        signal.shape[0] == 1
        and seqs % 2 == 0
        and rows % 128 == 0
        and channels % (8 * groups * seqs) == 0
    )


def angle_table(height, width, period):
    product = lax.broadcasted_iota(jnp.int32, (height, width), 0) * lax.broadcasted_iota(
        jnp.int32, (height, width), 1
    )
    return 2.0 * jnp.pi / period * (product % period).astype(jnp.float32)


def angle_of(product, period):
    return 2.0 * jnp.pi / period * (product % period).astype(jnp.float32)


def coarse_order(slot, seq_count):
    pair_index = slot // 2
    odd_slot = slot % 2
    return jnp.where(
        pair_index == 0,
        odd_slot * seq_count,
        jnp.where(odd_slot == 0, pair_index, 2 * seq_count - pair_index),
    )


def contract(form, table, operand):
    return jnp.einsum(form, table, operand, precision=lax.Precision.HIGHEST)


def forward_spectra(columns):
    seq_count = lax.axis_size("seq")
    row_count = columns.shape[0]
    part_rows = row_count // seq_count
    period_len = 2 * row_count * seq_count
    spread = lax.all_to_all(
        columns.reshape(1, row_count, columns.shape[1]),
        "seq",
        split_axis=1,
        concat_axis=0,
        tiled=True,
    )
    slot_grid = lax.broadcasted_iota(jnp.int32, (2 * seq_count, seq_count), 0)
    source_grid = lax.broadcasted_iota(jnp.int32, (2 * seq_count, seq_count), 1)
    first_table = angle_of(coarse_order(slot_grid, seq_count) * source_grid, 2 * seq_count)
    cos_first = jnp.cos(first_table)
    sin_first = jnp.sin(first_table)
    half_width = spread.shape[2] // 2
    real_in = spread[:, :, :half_width]
    imag_in = spread[:, :, half_width:]
    real_part = contract("ks,srw->krw", cos_first, real_in) + contract(
        "ks,srw->krw", sin_first, imag_in
    )
    imag_part = contract("ks,srw->krw", cos_first, imag_in) - contract(
        "ks,srw->krw", sin_first, real_in
    )
    global_row = lax.axis_index("seq") * part_rows + lax.broadcasted_iota(
        jnp.int32, (2 * seq_count, part_rows), 1
    )
    coarse = coarse_order(lax.broadcasted_iota(jnp.int32, (2 * seq_count, part_rows), 0), seq_count)
    phases = angle_of(global_row * coarse, period_len)
    cos_turn = jnp.cos(phases)[:, :, None]
    sin_turn = jnp.sin(phases)[:, :, None]
    rotated = jnp.stack(
        [real_part * cos_turn + imag_part * sin_turn, imag_part * cos_turn - real_part * sin_turn]
    )
    inner_table = angle_table(row_count, row_count, row_count)
    cos_inner = jnp.cos(inner_table)
    sin_inner = jnp.sin(inner_table)
    pieces = lax.all_to_all(rotated, "seq", split_axis=1, concat_axis=2, tiled=True)
    real_sum = contract("qr,krw->kqw", cos_inner, pieces[0]) + contract(
        "qr,krw->kqw", sin_inner, pieces[1]
    )
    imag_sum = contract("qr,krw->kqw", cos_inner, pieces[1]) - contract(
        "qr,krw->kqw", sin_inner, pieces[0]
    )
    return jnp.stack([real_sum, imag_sum])


def split_pairs(packed):
    reversed_q = packed[:, :, ::-1]
    zero_row = jnp.roll(reversed_q[:, 0], 1, axis=1)
    own_pair = jnp.stack([zero_row, reversed_q[:, 1]], axis=1)
    partner = jnp.where(lax.axis_index("seq") == 0, own_pair, reversed_q[:, ::-1])
    first = jnp.stack([0.5 * (packed[0] + partner[0]), 0.5 * (packed[1] - partner[1])])
    second = jnp.stack([0.5 * (packed[1] + partner[1]), 0.5 * (partner[0] - packed[0])])
    return (first, second)


def inverse_rows(spectra):
    seq_count = lax.axis_size("seq")
    row_count = spectra.shape[2]
    period_len = 2 * row_count * seq_count
    inner_table = angle_table(row_count, row_count, row_count)
    cos_inner = jnp.cos(inner_table)
    sin_inner = jnp.sin(inner_table)
    real_sum = contract("qr,krw->kqw", cos_inner, spectra[0]) - contract(
        "qr,krw->kqw", sin_inner, spectra[1]
    )
    imag_sum = contract("qr,krw->kqw", cos_inner, spectra[1]) + contract(
        "qr,krw->kqw", sin_inner, spectra[0]
    )
    coarse = coarse_order(
        2 * lax.axis_index("seq") + lax.broadcasted_iota(jnp.int32, (2, row_count), 0), seq_count
    )
    position = lax.broadcasted_iota(jnp.int32, (2, row_count), 1)
    phases = angle_of(position * coarse, period_len)
    cos_turn = jnp.cos(phases)[:, :, None]
    sin_turn = jnp.sin(phases)[:, :, None]
    rotated = jnp.stack(
        [real_sum * cos_turn - imag_sum * sin_turn, real_sum * sin_turn + imag_sum * cos_turn]
    )
    target_grid = lax.broadcasted_iota(jnp.int32, (seq_count, 2 * seq_count), 0)
    slot_grid = lax.broadcasted_iota(jnp.int32, (seq_count, 2 * seq_count), 1)
    last_table = angle_of(target_grid * coarse_order(slot_grid, seq_count), 2 * seq_count)
    cos_last = jnp.cos(last_table)
    sin_last = jnp.sin(last_table)
    pieces = lax.all_to_all(rotated, "seq", split_axis=2, concat_axis=1, tiled=True)
    value = contract("sk,krw->srw", cos_last, pieces[0]) - contract(
        "sk,krw->srw", sin_last, pieces[1]
    )
    other = contract("sk,krw->srw", sin_last, pieces[0]) + contract(
        "sk,krw->srw", cos_last, pieces[1]
    )
    gathered = (value / period_len, other / period_len)
    gathered = jnp.concatenate([gathered[0], gathered[1]], axis=2)
    home_rows = lax.all_to_all(gathered, "seq", split_axis=0, concat_axis=1, tiled=True)
    return home_rows.reshape(row_count, home_rows.shape[2])


def invert_all(spectra):
    half_width = spectra.shape[3] // 2
    joined = jnp.stack(
        [
            spectra[0, :, :, :half_width] - spectra[1, :, :, half_width:],
            spectra[1, :, :, :half_width] + spectra[0, :, :, half_width:],
        ]
    )
    return inverse_rows(joined)


def shards(signal, grad_out, filter_taps, skip_gain):
    channels = filter_taps.shape[1]
    signal_rows = signal[0].astype(jnp.float32)
    grad_rows = grad_out[0].astype(jnp.float32)
    tap_half = filter_taps.shape[1] // 2
    columns = jnp.concatenate(
        [signal_rows, filter_taps[:, :tap_half], grad_rows, filter_taps[:, tap_half:]], axis=1
    )
    first, second = split_pairs(forward_spectra(columns))
    signal_spec = first[:, :, :, :channels]
    grad_spec = second[:, :, :, :channels]
    own_spec = jnp.concatenate([first[:, :, :, channels:], second[:, :, :, channels:]], axis=3)
    input_spec = jnp.stack(
        [
            grad_spec[0] * own_spec[0] + grad_spec[1] * own_spec[1],
            grad_spec[1] * own_spec[0] - grad_spec[0] * own_spec[1],
        ]
    )
    filter_terms = jnp.stack(
        [
            grad_spec[0] * signal_spec[0] + grad_spec[1] * signal_spec[1],
            grad_spec[1] * signal_spec[0] - grad_spec[0] * signal_spec[1],
        ]
    )
    summed = lax.psum(filter_terms, "batch")
    rows_back = invert_all(jnp.concatenate([input_spec, summed], axis=3))
    filter_grad = rows_back[:, channels:]
    input_grad = (rows_back[:, :channels] + skip_gain[None, :] * grad_rows).astype(jnp.bfloat16)
    return (input_grad[None], filter_grad)


def solution(mesh):
    groups, seqs = mesh.shape["batch"], mesh.shape["seq"]

    def either(signal, grad_out, filter_taps, skip_gain):
        if fits_fused(groups, seqs, signal, filter_taps):
            return fused_shards(groups, seqs, signal, grad_out, filter_taps, skip_gain)
        return shards(signal, grad_out, filter_taps, skip_gain)

    return jax.shard_map(
        either,
        mesh=mesh,
        in_specs=(P("batch", "seq", None), P("batch", "seq", None), P("seq", None), P()),
        out_specs=(P("batch", "seq", None), P("seq", None)),
        check_vma=False,
    )
```

```python
import functools
import math

import jax
import jax.numpy as jnp
import numpy as np
from jax import lax
from jax.experimental import pallas as pl
from jax.experimental.pallas import tpu as pltpu
from jax.sharding import PartitionSpec as P

MESH = pl.DeviceIdType.MESH
F32 = jnp.float32
BF16 = jnp.bfloat16
GRAD, TAPS, SIGNAL, INPUT, FILTER, FORWARD = range(6)


def weighted(terms):
    total = None
    for factor, array in terms:
        if array is None or abs(factor) < 1e-12:
            continue
        if total is None:
            if abs(factor - 1.0) < 1e-12:
                total = array
            else:
                total = array * factor
        elif abs(factor - 1.0) < 1e-12:
            total = total + array
        elif abs(factor + 1.0) < 1e-12:
            total = total - array
        else:
            total = total + array * factor
    return total


def added(left, right):
    return weighted([(1.0, left), (1.0, right)])


def subtracted(left, right):
    return weighted([(1.0, left), (-1.0, right)])


def turn(real, imag, cos_turn, sin_turn):
    if imag is None:
        return real * cos_turn, -(real * sin_turn)
    return real * cos_turn + imag * sin_turn, imag * cos_turn - real * sin_turn


def coarse_forward(blocks):
    count = len(blocks)
    result = [None] * (count + 1)
    for k in range(count // 2 + 1):
        sums = []
        for parity in (0, 1):
            angles = [(math.pi * ((s * k) % (2 * count)) / count, s) for s in range(parity, count, 2)]
            sums.append(
                (
                    weighted([(math.cos(a), blocks[s]) for a, s in angles]),
                    weighted([(-math.sin(a), blocks[s]) for a, s in angles]),
                )
            )
        (even_re, even_im), (odd_re, odd_im) = sums
        result[k] = (added(even_re, odd_re), added(even_im, odd_im))
        if k != count - k:
            result[count - k] = (subtracted(even_re, odd_re), subtracted(odd_im, even_im))
    return result


def coarse_inverse(terms, scale):
    count = len(terms) - 1
    pairs = []
    for k in range(count // 2 + 1):
        weight = scale if k == 0 else 2.0 * scale
        real, imag = terms[k]
        if k == count - k:
            pairs.append((weight, real, imag, real, imag))
        else:
            other_re, other_im = terms[count - k]
            pairs.append((weight, real + other_re, imag - other_im, real - other_re, imag + other_im))
    blocks = []
    for s in range(count):
        parts = []
        for k, (weight, even_re, even_im, odd_re, odd_im) in enumerate(pairs):
            angle = math.pi * ((s * k) % (2 * count)) / count
            parts.append((weight * math.cos(angle) * (1 if abs(math.cos(angle)) > 1e-9 else 0), odd_re if s % 2 else even_re))
            parts.append((weight * math.sin(angle) * (1 if abs(math.sin(angle)) > 1e-9 else 0), odd_im if s % 2 else even_im))
        blocks.append(weighted(parts))
    return blocks


def fused_kernel(
    groups, seqs,
    signal_hbm, grad_hbm, tap_hbm, skip_hbm, high_hbm, low_hbm, cos_hbm, sin_hbm,
    input_ref, filter_ref,
    signal_ref, grad_ref, tap_ref, skip_ref, high_ref, low_ref, cos_ref, sin_ref,
    grad_out_buf, signal_out_buf, tap_out_buf, grad_in, signal_in, tap_in,
    input_out, filter_out, input_in, filter_in,
    grad_rows, grad_spec, signal_rows, signal_spec, input_rows, filter_rows, filter_spec,
    send_sems, recv_sems, load_sems,
):
    count = groups * seqs
    coarse = seqs + 1
    own, rows = grad_in.shape[1:]
    channels = count * own
    group, seq = lax.axis_index("batch"), lax.axis_index("seq")
    me = group * seqs + seq
    scale = 1.0 / (2 * seqs * rows)
    re, im = pl.ds(0, rows), pl.ds(rows, rows)

    parity, pair = lax.rem(group, 2), lax.div(group, 2)
    half_seqs, half_groups = seqs // 2, groups // 2
    upper, inner = lax.div(seq, half_seqs), lax.rem(seq, half_seqs)

    def load(index, source, target):
        return pltpu.make_async_copy(source, target, load_sems.at[index])

    loads = [
        load(index, source, target)
        for index, (source, target) in enumerate(
            (
                (grad_hbm, grad_ref), (tap_hbm, tap_ref), (signal_hbm, signal_ref),
                (cos_hbm, cos_ref), (sin_hbm, sin_ref), (high_hbm, high_ref),
                (low_hbm, low_ref), (skip_hbm, skip_ref),
            )
        )
    ]
    for copy in loads:
        copy.start()

    def seq_at(step):
        other = lax.rem(upper + 1 + lax.div(step, half_seqs), 2)
        return other * half_seqs + lax.rem(inner + step, half_seqs)

    def peer(step):
        to_seq = seq_at(lax.div(step, groups))
        to_group = lax.rem(group + step, groups)
        return to_group * seqs + to_seq, to_group, to_seq

    def over_peers(body, total, own_step):
        lax.fori_loop(0, own_step, body, 0)
        lax.fori_loop(own_step + 1, total, body, 0)

    barrier = pltpu.get_barrier_semaphore()

    def greet(step, carry):
        _, to_group, to_seq = peer(step)
        pl.semaphore_signal(
            barrier, inc=1, device_id={"batch": to_group, "seq": to_seq}, device_id_type=MESH
        )
        return carry

    over_peers(greet, count, half_seqs * groups)

    def transfer(source, target, kind, to_group, to_seq):
        return pltpu.make_async_remote_copy(
            src_ref=source,
            dst_ref=target,
            send_sem=send_sems.at[kind],
            recv_sem=recv_sems.at[kind],
            device_id={"batch": to_group, "seq": to_seq},
            device_id_type=MESH,
        )

    def all_of(buffer, blocks, kind):
        _, to_group, to_seq = peer(0)
        view = buffer.at[pl.ds(0, blocks)]
        return transfer(view, view, kind, to_group, to_seq)

    loads[GRAD].wait()
    grad_out_buf[...] = grad_ref[...].astype(F32).T.reshape(count, own, rows)
    loads[TAPS].wait()
    tap_out_buf[...] = tap_ref[...].T.reshape(count, own, rows)
    pl.semaphore_wait(barrier, count - 1)

    def send_taps(step, carry):
        to_seq = seq_at(step)
        place = group * seqs + to_seq
        transfer(tap_out_buf.at[place], tap_in.at[seq], TAPS, group, to_seq).start()
        return carry

    def send_grads(step, carry):
        place, to_group, to_seq = peer(step)
        transfer(grad_out_buf.at[place], grad_in.at[me], GRAD, to_group, to_seq).start()
        return carry

    def send_signals(step, carry):
        place, to_group, to_seq = peer(step)
        transfer(signal_out_buf.at[place], signal_in.at[me], SIGNAL, to_group, to_seq).start()
        return carry

    over_peers(send_taps, seqs, half_seqs)
    over_peers(send_grads, count, half_seqs * groups)
    loads[SIGNAL].wait()
    signal_out_buf[...] = signal_ref[...].astype(F32).T.reshape(count, own, rows)
    over_peers(send_signals, count, half_seqs * groups)
    grad_in[me] = grad_out_buf[me]
    tap_in[seq] = tap_out_buf[me]
    signal_in[me] = signal_out_buf[me]

    def spread(blocks, target, first_row):
        place = pl.ds(first_row, own)
        for k, (real, imag) in enumerate(coarse_forward(blocks)):
            real, imag = turn(real, imag, cos_ref[k], sin_ref[k])
            target[k, place, re] = real
            target[k, place, im] = imag

    def fine(source, target):
        lines = source.shape[0] * source.shape[1]
        value = source[...].reshape(lines, 2 * rows)
        high = value.astype(BF16)
        low = (value - high.astype(F32)).astype(BF16)
        product = functools.partial(jnp.dot, preferred_element_type=F32)
        total = product(high, high_ref[...]) + product(low, high_ref[...]) + product(high, low_ref[...])
        target[...] = total.reshape(target.shape)

    def collect(source, first_row):
        place = pl.ds(first_row, own)
        terms = [
            turn(source[k, place, re], source[k, place, im], cos_ref[k], sin_ref[k])
            for k in range(coarse)
        ]
        return coarse_inverse(terms, scale)

    def row_of(index):
        return pl.multiple_of(index * own, own)

    for copy in loads[3:]:
        copy.wait()
    all_of(tap_in, seqs - 1, TAPS).wait_recv()
    spread([tap_in[s] for s in range(seqs)], grad_rows, groups * own)
    all_of(grad_in, count - 1, GRAD).wait_recv()

    def spread_grad(index, carry):
        spread([grad_in[index * seqs + s] for s in range(seqs)], grad_rows, row_of(index))
        return carry

    lax.fori_loop(0, groups, spread_grad, 0)
    fine(grad_rows, grad_spec)

    def multiply_taps(index, carry):
        place, fixed = pl.ds(row_of(index), own), pl.ds(groups * own, own)
        for k in range(coarse):
            grad_re, grad_im = grad_spec[k, place, re], grad_spec[k, place, im]
            tap_re, tap_im = grad_spec[k, fixed, re], grad_spec[k, fixed, im]
            input_rows[k, place, re] = grad_re * tap_re + grad_im * tap_im
            input_rows[k, place, im] = grad_re * tap_im - grad_im * tap_re
        return carry

    lax.fori_loop(0, groups, multiply_taps, 0)
    fine(input_rows, input_rows)

    def collect_input(index, carry):
        for s, block in enumerate(collect(input_rows, row_of(index))):
            input_out[index * seqs + s] = block
        return carry

    lax.fori_loop(0, groups, collect_input, 0)

    def send_inputs(step, carry):
        place, to_group, to_seq = peer(step)
        transfer(input_out.at[place], input_in.at[me], INPUT, to_group, to_seq).start()
        return carry

    over_peers(send_inputs, count, half_seqs * groups)
    input_in[me] = input_out[me]

    all_of(signal_in, count - 1, SIGNAL).wait_recv()

    def spread_signal(index, carry):
        spread([signal_in[index * seqs + s] for s in range(seqs)], signal_rows, row_of(index))
        return carry

    lax.fori_loop(0, groups, spread_signal, 0)
    fine(signal_rows, signal_spec)
    for k in range(coarse):
        real, imag = None, None
        for index in range(groups):
            place = pl.ds(index * own, own)
            grad_re, grad_im = grad_spec[k, place, re], grad_spec[k, place, im]
            signal_re, signal_im = signal_spec[k, place, re], signal_spec[k, place, im]
            real = added(real, grad_re * signal_re + grad_im * signal_im)
            imag = added(imag, grad_re * signal_im - grad_im * signal_re)
        filter_rows[k, :, re] = real
        filter_rows[k, :, im] = imag
    fine(filter_rows, filter_spec)
    for s, block in enumerate(collect(filter_spec, 0)):
        filter_out[s] = block

    def send_filters(step, carry):
        to_seq = seq_at(lax.div(step, half_groups))
        to_group = 2 * lax.rem(pair + step, half_groups) + parity
        place = pair * seqs + seq
        transfer(
            filter_out.at[to_seq], filter_in.at[parity, place], FILTER, to_group, to_seq
        ).start()
        return carry

    over_peers(send_filters, seqs * half_groups, half_seqs * half_groups)
    filter_in[parity, pair * seqs + seq] = filter_out[seq]

    half = count // 2
    all_of(input_in, count - 1, INPUT).wait_recv()
    gradient = input_in[...].reshape(channels, rows).T + skip_ref[...] * grad_ref[...].astype(F32)
    input_ref[...] = gradient.astype(BF16)
    all_of(filter_in.at[0], half - 1, FILTER).wait_recv()
    mine = filter_in.at[parity]
    partner = 2 * pair + 1 - parity
    forward = transfer(mine, mine, FORWARD, partner, seq)
    forward.start()
    forward.wait_recv()
    parts = [
        filter_in[which, first * seqs : (first + 1) * seqs].reshape(seqs * own, rows)
        for first in range(half_groups)
        for which in range(2)
    ]
    filter_ref[...] = jnp.concatenate(parts, axis=0).T
    for kind, buffer in ((GRAD, grad_in), (SIGNAL, signal_in), (INPUT, input_in)):
        all_of(buffer, count - 1, kind).wait_send()
    all_of(filter_in.at[0], half - 1, FILTER).wait_send()
    forward.wait_send()
    all_of(tap_in, seqs - 1, TAPS).wait_send()


def fine_tables(rows):
    grid = np.arange(rows)
    angle = 2.0 * np.pi / rows * (np.outer(grid, grid) % rows)
    table = np.block([[np.cos(angle), -np.sin(angle)], [np.sin(angle), np.cos(angle)]]).astype(np.float32)
    high = table.astype(BF16)
    return high, (table - high.astype(np.float32)).astype(BF16)


def turn_tables(seqs, rows, lines):
    angle = np.pi / (seqs * rows) * np.outer(np.arange(seqs + 1), np.arange(rows))
    wide = np.broadcast_to(angle[:, None, :], (seqs + 1, lines, rows))
    return np.cos(wide).astype(np.float32), np.sin(wide).astype(np.float32)


def fused_shards(groups, seqs, signal, grad_out, filter_taps, skip_gain):
    rows, channels = filter_taps.shape
    count, coarse = groups * seqs, seqs + 1
    own = channels // count
    high, low = fine_tables(rows)
    cos_turn, sin_turn = turn_tables(seqs, rows, own)
    blocks = pltpu.VMEM((count, own, rows), F32)
    few = pltpu.VMEM((seqs, own, rows), F32)
    lines = lambda number: pltpu.VMEM((coarse, number * own, 2 * rows), F32)
    vmem = pl.BlockSpec(memory_space=pltpu.VMEM)
    hbm = pl.BlockSpec(memory_space=pltpu.HBM)
    turns = pltpu.VMEM((coarse, own, rows), F32)
    table = pltpu.VMEM((2 * rows, 2 * rows), BF16)
    input_grad, filter_grad = pl.pallas_call(
        functools.partial(fused_kernel, groups, seqs),
        out_shape=(
            jax.ShapeDtypeStruct((rows, channels), BF16),
            jax.ShapeDtypeStruct((rows, channels), F32),
        ),
        in_specs=[hbm] * 8,
        out_specs=(vmem, vmem),
        scratch_shapes=[
            pltpu.VMEM((rows, channels), BF16), pltpu.VMEM((rows, channels), BF16),
            pltpu.VMEM((rows, channels), F32), pltpu.VMEM((1, channels), F32),
            table, table, turns, turns,
            blocks, blocks, blocks, blocks, blocks, few,
            blocks, few, blocks, pltpu.VMEM((2, count // 2, own, rows), F32),
            lines(groups + 1), lines(groups + 1), lines(groups), lines(groups),
            lines(groups), lines(1), lines(1),
            pltpu.SemaphoreType.DMA((6,)),
            pltpu.SemaphoreType.DMA((6,)),
            pltpu.SemaphoreType.DMA((8,)),
        ],
        compiler_params=pltpu.CompilerParams(
            collective_id=0, has_side_effects=True, vmem_limit_bytes=48 * 1024 * 1024
        ),
    )(
        signal[0], grad_out[0], filter_taps, skip_gain[None, :],
        jnp.asarray(high), jnp.asarray(low), jnp.asarray(cos_turn), jnp.asarray(sin_turn),
    )
    return input_grad[None], filter_grad


def fits_fused(groups, seqs, signal, filter_taps):
    rows, channels = filter_taps.shape
    return (
        signal.shape[0] == 1
        and seqs % 2 == 0
        and groups % 2 == 0
        and rows % 128 == 0
        and channels % (8 * groups * seqs) == 0
    )


def angle_table(height, width, period):
    product = lax.broadcasted_iota(jnp.int32, (height, width), 0) * lax.broadcasted_iota(
        jnp.int32, (height, width), 1
    )
    return 2.0 * jnp.pi / period * (product % period).astype(jnp.float32)


def angle_of(product, period):
    return 2.0 * jnp.pi / period * (product % period).astype(jnp.float32)


def coarse_order(slot, seq_count):
    pair_index = slot // 2
    odd_slot = slot % 2
    return jnp.where(
        pair_index == 0,
        odd_slot * seq_count,
        jnp.where(odd_slot == 0, pair_index, 2 * seq_count - pair_index),
    )


def contract(form, table, operand):
    return jnp.einsum(form, table, operand, precision=lax.Precision.HIGHEST)


def forward_spectra(columns):
    seq_count = lax.axis_size("seq")
    row_count = columns.shape[0]
    part_rows = row_count // seq_count
    period_len = 2 * row_count * seq_count
    spread = lax.all_to_all(
        columns.reshape(1, row_count, columns.shape[1]),
        "seq",
        split_axis=1,
        concat_axis=0,
        tiled=True,
    )
    slot_grid = lax.broadcasted_iota(jnp.int32, (2 * seq_count, seq_count), 0)
    source_grid = lax.broadcasted_iota(jnp.int32, (2 * seq_count, seq_count), 1)
    first_table = angle_of(coarse_order(slot_grid, seq_count) * source_grid, 2 * seq_count)
    cos_first = jnp.cos(first_table)
    sin_first = jnp.sin(first_table)
    half_width = spread.shape[2] // 2
    real_in = spread[:, :, :half_width]
    imag_in = spread[:, :, half_width:]
    real_part = contract("ks,srw->krw", cos_first, real_in) + contract(
        "ks,srw->krw", sin_first, imag_in
    )
    imag_part = contract("ks,srw->krw", cos_first, imag_in) - contract(
        "ks,srw->krw", sin_first, real_in
    )
    global_row = lax.axis_index("seq") * part_rows + lax.broadcasted_iota(
        jnp.int32, (2 * seq_count, part_rows), 1
    )
    coarse = coarse_order(lax.broadcasted_iota(jnp.int32, (2 * seq_count, part_rows), 0), seq_count)
    phases = angle_of(global_row * coarse, period_len)
    cos_turn = jnp.cos(phases)[:, :, None]
    sin_turn = jnp.sin(phases)[:, :, None]
    rotated = jnp.stack(
        [real_part * cos_turn + imag_part * sin_turn, imag_part * cos_turn - real_part * sin_turn]
    )
    inner_table = angle_table(row_count, row_count, row_count)
    cos_inner = jnp.cos(inner_table)
    sin_inner = jnp.sin(inner_table)
    pieces = lax.all_to_all(rotated, "seq", split_axis=1, concat_axis=2, tiled=True)
    real_sum = contract("qr,krw->kqw", cos_inner, pieces[0]) + contract(
        "qr,krw->kqw", sin_inner, pieces[1]
    )
    imag_sum = contract("qr,krw->kqw", cos_inner, pieces[1]) - contract(
        "qr,krw->kqw", sin_inner, pieces[0]
    )
    return jnp.stack([real_sum, imag_sum])


def split_pairs(packed):
    reversed_q = packed[:, :, ::-1]
    zero_row = jnp.roll(reversed_q[:, 0], 1, axis=1)
    own_pair = jnp.stack([zero_row, reversed_q[:, 1]], axis=1)
    partner = jnp.where(lax.axis_index("seq") == 0, own_pair, reversed_q[:, ::-1])
    first = jnp.stack([0.5 * (packed[0] + partner[0]), 0.5 * (packed[1] - partner[1])])
    second = jnp.stack([0.5 * (packed[1] + partner[1]), 0.5 * (partner[0] - packed[0])])
    return (first, second)


def inverse_rows(spectra):
    seq_count = lax.axis_size("seq")
    row_count = spectra.shape[2]
    period_len = 2 * row_count * seq_count
    inner_table = angle_table(row_count, row_count, row_count)
    cos_inner = jnp.cos(inner_table)
    sin_inner = jnp.sin(inner_table)
    real_sum = contract("qr,krw->kqw", cos_inner, spectra[0]) - contract(
        "qr,krw->kqw", sin_inner, spectra[1]
    )
    imag_sum = contract("qr,krw->kqw", cos_inner, spectra[1]) + contract(
        "qr,krw->kqw", sin_inner, spectra[0]
    )
    coarse = coarse_order(
        2 * lax.axis_index("seq") + lax.broadcasted_iota(jnp.int32, (2, row_count), 0), seq_count
    )
    position = lax.broadcasted_iota(jnp.int32, (2, row_count), 1)
    phases = angle_of(position * coarse, period_len)
    cos_turn = jnp.cos(phases)[:, :, None]
    sin_turn = jnp.sin(phases)[:, :, None]
    rotated = jnp.stack(
        [real_sum * cos_turn - imag_sum * sin_turn, real_sum * sin_turn + imag_sum * cos_turn]
    )
    target_grid = lax.broadcasted_iota(jnp.int32, (seq_count, 2 * seq_count), 0)
    slot_grid = lax.broadcasted_iota(jnp.int32, (seq_count, 2 * seq_count), 1)
    last_table = angle_of(target_grid * coarse_order(slot_grid, seq_count), 2 * seq_count)
    cos_last = jnp.cos(last_table)
    sin_last = jnp.sin(last_table)
    pieces = lax.all_to_all(rotated, "seq", split_axis=2, concat_axis=1, tiled=True)
    value = contract("sk,krw->srw", cos_last, pieces[0]) - contract(
        "sk,krw->srw", sin_last, pieces[1]
    )
    other = contract("sk,krw->srw", sin_last, pieces[0]) + contract(
        "sk,krw->srw", cos_last, pieces[1]
    )
    gathered = (value / period_len, other / period_len)
    gathered = jnp.concatenate([gathered[0], gathered[1]], axis=2)
    home_rows = lax.all_to_all(gathered, "seq", split_axis=0, concat_axis=1, tiled=True)
    return home_rows.reshape(row_count, home_rows.shape[2])


def invert_all(spectra):
    half_width = spectra.shape[3] // 2
    joined = jnp.stack(
        [
            spectra[0, :, :, :half_width] - spectra[1, :, :, half_width:],
            spectra[1, :, :, :half_width] + spectra[0, :, :, half_width:],
        ]
    )
    return inverse_rows(joined)


def shards(signal, grad_out, filter_taps, skip_gain):
    channels = filter_taps.shape[1]
    signal_rows = signal[0].astype(jnp.float32)
    grad_rows = grad_out[0].astype(jnp.float32)
    tap_half = filter_taps.shape[1] // 2
    columns = jnp.concatenate(
        [signal_rows, filter_taps[:, :tap_half], grad_rows, filter_taps[:, tap_half:]], axis=1
    )
    first, second = split_pairs(forward_spectra(columns))
    signal_spec = first[:, :, :, :channels]
    grad_spec = second[:, :, :, :channels]
    own_spec = jnp.concatenate([first[:, :, :, channels:], second[:, :, :, channels:]], axis=3)
    input_spec = jnp.stack(
        [
            grad_spec[0] * own_spec[0] + grad_spec[1] * own_spec[1],
            grad_spec[1] * own_spec[0] - grad_spec[0] * own_spec[1],
        ]
    )
    filter_terms = jnp.stack(
        [
            grad_spec[0] * signal_spec[0] + grad_spec[1] * signal_spec[1],
            grad_spec[1] * signal_spec[0] - grad_spec[0] * signal_spec[1],
        ]
    )
    summed = lax.psum(filter_terms, "batch")
    rows_back = invert_all(jnp.concatenate([input_spec, summed], axis=3))
    filter_grad = rows_back[:, channels:]
    input_grad = (rows_back[:, :channels] + skip_gain[None, :] * grad_rows).astype(jnp.bfloat16)
    return (input_grad[None], filter_grad)


def solution(mesh):
    groups, seqs = mesh.shape["batch"], mesh.shape["seq"]

    def either(signal, grad_out, filter_taps, skip_gain):
        if fits_fused(groups, seqs, signal, filter_taps):
            return fused_shards(groups, seqs, signal, grad_out, filter_taps, skip_gain)
        return shards(signal, grad_out, filter_taps, skip_gain)

    return jax.shard_map(
        either,
        mesh=mesh,
        in_specs=(P("batch", "seq", None), P("batch", "seq", None), P("seq", None), P()),
        out_specs=(P("batch", "seq", None), P("seq", None)),
        check_vma=False,
    )
```

```python
import functools
import math

import jax
import jax.numpy as jnp
import numpy as np
from jax import lax
from jax.experimental import pallas as pl
from jax.experimental.pallas import tpu as pltpu
from jax.sharding import PartitionSpec as P

MESH = pl.DeviceIdType.MESH
F32 = jnp.float32
BF16 = jnp.bfloat16
GRAD, TAPS, SIGNAL, INPUT, FILTER, FORWARD = range(6)


def weighted(terms):
    total = None
    for factor, array in terms:
        if array is None or abs(factor) < 1e-12:
            continue
        if total is None:
            if abs(factor - 1.0) < 1e-12:
                total = array
            else:
                total = array * factor
        elif abs(factor - 1.0) < 1e-12:
            total = total + array
        elif abs(factor + 1.0) < 1e-12:
            total = total - array
        else:
            total = total + array * factor
    return total


def added(left, right):
    return weighted([(1.0, left), (1.0, right)])


def subtracted(left, right):
    return weighted([(1.0, left), (-1.0, right)])


def turn(real, imag, cos_turn, sin_turn):
    if imag is None:
        return real * cos_turn, -(real * sin_turn)
    return real * cos_turn + imag * sin_turn, imag * cos_turn - real * sin_turn


def coarse_forward(blocks):
    count = len(blocks)
    result = [None] * (count + 1)
    for k in range(count // 2 + 1):
        sums = []
        for parity in (0, 1):
            angles = [(math.pi * ((s * k) % (2 * count)) / count, s) for s in range(parity, count, 2)]
            sums.append(
                (
                    weighted([(math.cos(a), blocks[s]) for a, s in angles]),
                    weighted([(-math.sin(a), blocks[s]) for a, s in angles]),
                )
            )
        (even_re, even_im), (odd_re, odd_im) = sums
        result[k] = (added(even_re, odd_re), added(even_im, odd_im))
        if k != count - k:
            result[count - k] = (subtracted(even_re, odd_re), subtracted(odd_im, even_im))
    return result


def coarse_inverse(terms, scale):
    count = len(terms) - 1
    pairs = []
    for k in range(count // 2 + 1):
        weight = scale if k == 0 else 2.0 * scale
        real, imag = terms[k]
        if k == count - k:
            pairs.append((weight, real, imag, real, imag))
        else:
            other_re, other_im = terms[count - k]
            pairs.append((weight, real + other_re, imag - other_im, real - other_re, imag + other_im))
    blocks = []
    for s in range(count):
        parts = []
        for k, (weight, even_re, even_im, odd_re, odd_im) in enumerate(pairs):
            angle = math.pi * ((s * k) % (2 * count)) / count
            parts.append((weight * math.cos(angle) * (1 if abs(math.cos(angle)) > 1e-9 else 0), odd_re if s % 2 else even_re))
            parts.append((weight * math.sin(angle) * (1 if abs(math.sin(angle)) > 1e-9 else 0), odd_im if s % 2 else even_im))
        blocks.append(weighted(parts))
    return blocks


def fused_kernel(
    groups, seqs,
    signal_hbm, grad_hbm, tap_hbm, skip_hbm, high_hbm, low_hbm, cos_hbm, sin_hbm,
    input_ref, filter_ref,
    signal_ref, grad_ref, tap_ref, skip_ref, high_ref, low_ref, cos_ref, sin_ref,
    grad_out_buf, signal_out_buf, tap_out_buf, grad_in, signal_in, tap_in,
    input_out, filter_out, input_in, filter_in,
    grad_rows, grad_spec, signal_rows, signal_spec, input_rows, filter_rows, filter_spec,
    send_sems, recv_sems, load_sems,
):
    count = groups * seqs
    coarse = seqs + 1
    own, rows = grad_in.shape[1:]
    channels = count * own
    group, seq = lax.axis_index("batch"), lax.axis_index("seq")
    me = group * seqs + seq
    scale = 1.0 / (2 * seqs * rows)
    re, im = pl.ds(0, rows), pl.ds(rows, rows)

    parity, pair = lax.rem(group, 2), lax.div(group, 2)
    half_seqs, half_groups = seqs // 2, groups // 2
    upper, inner = lax.div(seq, half_seqs), lax.rem(seq, half_seqs)

    def load(index, source, target):
        return pltpu.make_async_copy(source, target, load_sems.at[index])

    loads = [
        load(index, source, target)
        for index, (source, target) in enumerate(
            (
                (grad_hbm, grad_ref), (tap_hbm, tap_ref), (signal_hbm, signal_ref),
                (cos_hbm, cos_ref), (sin_hbm, sin_ref), (high_hbm, high_ref),
                (low_hbm, low_ref), (skip_hbm, skip_ref),
            )
        )
    ]
    for copy in loads:
        copy.start()

    def seq_at(step):
        other = lax.rem(upper + 1 + lax.div(step, half_seqs), 2)
        return other * half_seqs + lax.rem(inner + step, half_seqs)

    def peer(step):
        to_seq = seq_at(lax.div(step, groups))
        to_group = lax.rem(group + step, groups)
        return to_group * seqs + to_seq, to_group, to_seq

    def over_peers(body, total, own_step):
        lax.fori_loop(0, own_step, body, 0)
        lax.fori_loop(own_step + 1, total, body, 0)

    barrier = pltpu.get_barrier_semaphore()

    def greet(step, carry):
        _, to_group, to_seq = peer(step)
        pl.semaphore_signal(
            barrier, inc=1, device_id={"batch": to_group, "seq": to_seq}, device_id_type=MESH
        )
        return carry

    over_peers(greet, count, half_seqs * groups)

    def transfer(source, target, kind, to_group, to_seq):
        return pltpu.make_async_remote_copy(
            src_ref=source,
            dst_ref=target,
            send_sem=send_sems.at[kind],
            recv_sem=recv_sems.at[kind],
            device_id={"batch": to_group, "seq": to_seq},
            device_id_type=MESH,
        )

    def all_of(buffer, blocks, kind):
        _, to_group, to_seq = peer(0)
        view = buffer.at[pl.ds(0, blocks)]
        return transfer(view, view, kind, to_group, to_seq)

    loads[GRAD].wait()
    grad_out_buf[...] = grad_ref[...].astype(F32).T.reshape(count, own, rows)
    loads[TAPS].wait()
    tap_out_buf[...] = tap_ref[...].T.reshape(count, own, rows)
    pl.semaphore_wait(barrier, count - 1)

    def send_taps(step, carry):
        to_seq = seq_at(step)
        place = group * seqs + to_seq
        transfer(tap_out_buf.at[place], tap_in.at[seq], TAPS, group, to_seq).start()
        return carry

    def send_grads(step, carry):
        place, to_group, to_seq = peer(step)
        transfer(grad_out_buf.at[place], grad_in.at[me], GRAD, to_group, to_seq).start()
        return carry

    def send_signals(step, carry):
        place, to_group, to_seq = peer(step)
        transfer(signal_out_buf.at[place], signal_in.at[me], SIGNAL, to_group, to_seq).start()
        return carry

    over_peers(send_taps, seqs, half_seqs)
    over_peers(send_grads, count, half_seqs * groups)
    loads[SIGNAL].wait()
    signal_out_buf[...] = signal_ref[...].astype(F32).T.reshape(count, own, rows)
    over_peers(send_signals, count, half_seqs * groups)
    grad_in[me] = grad_out_buf[me]
    tap_in[seq] = tap_out_buf[me]
    signal_in[me] = signal_out_buf[me]

    def spread(blocks, target, first_row):
        place = pl.ds(first_row, own)
        for k, (real, imag) in enumerate(coarse_forward(blocks)):
            real, imag = turn(real, imag, cos_ref[k], sin_ref[k])
            target[k, place, re] = real
            target[k, place, im] = imag

    def fine(source, target):
        lines = source.shape[0] * source.shape[1]
        value = source[...].reshape(lines, 2 * rows)
        high = value.astype(BF16)
        low = (value - high.astype(F32)).astype(BF16)
        product = functools.partial(jnp.dot, preferred_element_type=F32)
        total = product(high, high_ref[...]) + product(low, high_ref[...]) + product(high, low_ref[...])
        target[...] = total.reshape(target.shape)

    def collect(source, first_row):
        place = pl.ds(first_row, own)
        terms = [
            turn(source[k, place, re], source[k, place, im], cos_ref[k], sin_ref[k])
            for k in range(coarse)
        ]
        return coarse_inverse(terms, scale)

    def row_of(index):
        return pl.multiple_of(index * own, own)

    for copy in loads[3:]:
        copy.wait()
    all_of(tap_in, seqs - 1, TAPS).wait_recv()
    spread([tap_in[s] for s in range(seqs)], grad_rows, groups * own)
    all_of(grad_in, count - 1, GRAD).wait_recv()

    def spread_grad(index, carry):
        spread([grad_in[index * seqs + s] for s in range(seqs)], grad_rows, row_of(index))
        return carry

    lax.fori_loop(0, groups, spread_grad, 0)
    fine(grad_rows, grad_spec)

    def multiply_taps(index, carry):
        place, fixed = pl.ds(row_of(index), own), pl.ds(groups * own, own)
        for k in range(coarse):
            grad_re, grad_im = grad_spec[k, place, re], grad_spec[k, place, im]
            tap_re, tap_im = grad_spec[k, fixed, re], grad_spec[k, fixed, im]
            input_rows[k, place, re] = grad_re * tap_re + grad_im * tap_im
            input_rows[k, place, im] = grad_re * tap_im - grad_im * tap_re
        return carry

    lax.fori_loop(0, groups, multiply_taps, 0)
    fine(input_rows, input_rows)

    def collect_input(index, carry):
        for s, block in enumerate(collect(input_rows, row_of(index))):
            input_out[index * seqs + s] = block
        return carry

    lax.fori_loop(0, groups, collect_input, 0)

    def send_inputs(step, carry):
        place, to_group, to_seq = peer(step)
        transfer(input_out.at[place], input_in.at[me], INPUT, to_group, to_seq).start()
        return carry

    over_peers(send_inputs, count, half_seqs * groups)
    input_in[me] = input_out[me]

    all_of(signal_in, count - 1, SIGNAL).wait_recv()

    def spread_signal(index, carry):
        spread([signal_in[index * seqs + s] for s in range(seqs)], signal_rows, row_of(index))
        return carry

    lax.fori_loop(0, groups, spread_signal, 0)
    fine(signal_rows, signal_spec)
    for k in range(coarse):
        real, imag = None, None
        for index in range(groups):
            place = pl.ds(index * own, own)
            grad_re, grad_im = grad_spec[k, place, re], grad_spec[k, place, im]
            signal_re, signal_im = signal_spec[k, place, re], signal_spec[k, place, im]
            real = added(real, grad_re * signal_re + grad_im * signal_im)
            imag = added(imag, grad_re * signal_im - grad_im * signal_re)
        filter_rows[k, :, re] = real
        filter_rows[k, :, im] = imag
    fine(filter_rows, filter_spec)
    for s, block in enumerate(collect(filter_spec, 0)):
        filter_out[s] = block

    def send_filters(step, carry):
        to_seq = seq_at(lax.div(step, half_groups))
        to_group = 2 * lax.rem(pair + step, half_groups) + parity
        place = pair * seqs + seq
        transfer(
            filter_out.at[to_seq], filter_in.at[parity, place], FILTER, to_group, to_seq
        ).start()
        return carry

    over_peers(send_filters, seqs * half_groups, half_seqs * half_groups)
    filter_in[parity, pair * seqs + seq] = filter_out[seq]

    half = count // 2
    all_of(input_in, count - 1, INPUT).wait_recv()
    gradient = input_in[...].reshape(channels, rows).T + skip_ref[...] * grad_ref[...].astype(F32)
    input_ref[...] = gradient.astype(BF16)
    all_of(filter_in.at[0], half - 1, FILTER).wait_recv()
    mine = filter_in.at[parity]
    partner = 2 * pair + 1 - parity
    forward = transfer(mine, mine, FORWARD, partner, seq)
    forward.start()
    forward.wait_recv()
    parts = [
        filter_in[which, first * seqs : (first + 1) * seqs].reshape(seqs * own, rows)
        for first in range(half_groups)
        for which in range(2)
    ]
    filter_ref[...] = jnp.concatenate(parts, axis=0).T
    for kind, buffer in ((GRAD, grad_in), (SIGNAL, signal_in), (INPUT, input_in)):
        all_of(buffer, count - 1, kind).wait_send()
    all_of(filter_in.at[0], half - 1, FILTER).wait_send()
    forward.wait_send()
    all_of(tap_in, seqs - 1, TAPS).wait_send()


def fine_tables(rows):
    grid = np.arange(rows)
    angle = 2.0 * np.pi / rows * (np.outer(grid, grid) % rows)
    table = np.block([[np.cos(angle), -np.sin(angle)], [np.sin(angle), np.cos(angle)]]).astype(np.float32)
    high = table.astype(BF16)
    return high, (table - high.astype(np.float32)).astype(BF16)


def turn_tables(seqs, rows, lines):
    angle = np.pi / (seqs * rows) * np.outer(np.arange(seqs + 1), np.arange(rows))
    wide = np.broadcast_to(angle[:, None, :], (seqs + 1, lines, rows))
    return np.cos(wide).astype(np.float32), np.sin(wide).astype(np.float32)


def fused_shards(groups, seqs, signal, grad_out, filter_taps, skip_gain):
    rows, channels = filter_taps.shape
    count, coarse = groups * seqs, seqs + 1
    own = channels // count
    high, low = fine_tables(rows)
    cos_turn, sin_turn = turn_tables(seqs, rows, own)
    blocks = pltpu.VMEM((count, own, rows), F32)
    few = pltpu.VMEM((seqs, own, rows), F32)
    lines = lambda number: pltpu.VMEM((coarse, number * own, 2 * rows), F32)
    vmem = pl.BlockSpec(memory_space=pltpu.VMEM)
    hbm = pl.BlockSpec(memory_space=pltpu.HBM)
    turns = pltpu.VMEM((coarse, own, rows), F32)
    table = pltpu.VMEM((2 * rows, 2 * rows), BF16)
    input_grad, filter_grad = pl.pallas_call(
        functools.partial(fused_kernel, groups, seqs),
        out_shape=(
            jax.ShapeDtypeStruct((rows, channels), BF16),
            jax.ShapeDtypeStruct((rows, channels), F32),
        ),
        in_specs=[hbm] * 8,
        out_specs=(vmem, vmem),
        scratch_shapes=[
            pltpu.VMEM((rows, channels), BF16), pltpu.VMEM((rows, channels), BF16),
            pltpu.VMEM((rows, channels), F32), pltpu.VMEM((1, channels), F32),
            table, table, turns, turns,
            blocks, blocks, blocks, blocks, blocks, few,
            blocks, few, blocks, pltpu.VMEM((2, count // 2, own, rows), F32),
            lines(groups + 1), lines(groups + 1), lines(groups), lines(groups),
            lines(groups), lines(1), lines(1),
            pltpu.SemaphoreType.DMA((6,)),
            pltpu.SemaphoreType.DMA((6,)),
            pltpu.SemaphoreType.DMA((8,)),
        ],
        compiler_params=pltpu.CompilerParams(
            collective_id=0, has_side_effects=True, vmem_limit_bytes=67_043_328
        ),
    )(
        signal[0], grad_out[0], filter_taps, skip_gain[None, :],
        jnp.asarray(high), jnp.asarray(low), jnp.asarray(cos_turn), jnp.asarray(sin_turn),
    )
    return input_grad[None], filter_grad


def fits_fused(groups, seqs, signal, filter_taps):
    rows, channels = filter_taps.shape
    return (
        signal.shape[0] == 1
        and seqs % 2 == 0
        and groups % 2 == 0
        and rows % 128 == 0
        and channels % (8 * groups * seqs) == 0
    )


def angle_table(height, width, period):
    product = lax.broadcasted_iota(jnp.int32, (height, width), 0) * lax.broadcasted_iota(
        jnp.int32, (height, width), 1
    )
    return 2.0 * jnp.pi / period * (product % period).astype(jnp.float32)


def angle_of(product, period):
    return 2.0 * jnp.pi / period * (product % period).astype(jnp.float32)


def coarse_order(slot, seq_count):
    pair_index = slot // 2
    odd_slot = slot % 2
    return jnp.where(
        pair_index == 0,
        odd_slot * seq_count,
        jnp.where(odd_slot == 0, pair_index, 2 * seq_count - pair_index),
    )


def contract(form, table, operand):
    return jnp.einsum(form, table, operand, precision=lax.Precision.HIGHEST)


def forward_spectra(columns):
    seq_count = lax.axis_size("seq")
    row_count = columns.shape[0]
    part_rows = row_count // seq_count
    period_len = 2 * row_count * seq_count
    spread = lax.all_to_all(
        columns.reshape(1, row_count, columns.shape[1]),
        "seq",
        split_axis=1,
        concat_axis=0,
        tiled=True,
    )
    slot_grid = lax.broadcasted_iota(jnp.int32, (2 * seq_count, seq_count), 0)
    source_grid = lax.broadcasted_iota(jnp.int32, (2 * seq_count, seq_count), 1)
    first_table = angle_of(coarse_order(slot_grid, seq_count) * source_grid, 2 * seq_count)
    cos_first = jnp.cos(first_table)
    sin_first = jnp.sin(first_table)
    half_width = spread.shape[2] // 2
    real_in = spread[:, :, :half_width]
    imag_in = spread[:, :, half_width:]
    real_part = contract("ks,srw->krw", cos_first, real_in) + contract(
        "ks,srw->krw", sin_first, imag_in
    )
    imag_part = contract("ks,srw->krw", cos_first, imag_in) - contract(
        "ks,srw->krw", sin_first, real_in
    )
    global_row = lax.axis_index("seq") * part_rows + lax.broadcasted_iota(
        jnp.int32, (2 * seq_count, part_rows), 1
    )
    coarse = coarse_order(lax.broadcasted_iota(jnp.int32, (2 * seq_count, part_rows), 0), seq_count)
    phases = angle_of(global_row * coarse, period_len)
    cos_turn = jnp.cos(phases)[:, :, None]
    sin_turn = jnp.sin(phases)[:, :, None]
    rotated = jnp.stack(
        [real_part * cos_turn + imag_part * sin_turn, imag_part * cos_turn - real_part * sin_turn]
    )
    inner_table = angle_table(row_count, row_count, row_count)
    cos_inner = jnp.cos(inner_table)
    sin_inner = jnp.sin(inner_table)
    pieces = lax.all_to_all(rotated, "seq", split_axis=1, concat_axis=2, tiled=True)
    real_sum = contract("qr,krw->kqw", cos_inner, pieces[0]) + contract(
        "qr,krw->kqw", sin_inner, pieces[1]
    )
    imag_sum = contract("qr,krw->kqw", cos_inner, pieces[1]) - contract(
        "qr,krw->kqw", sin_inner, pieces[0]
    )
    return jnp.stack([real_sum, imag_sum])


def split_pairs(packed):
    reversed_q = packed[:, :, ::-1]
    zero_row = jnp.roll(reversed_q[:, 0], 1, axis=1)
    own_pair = jnp.stack([zero_row, reversed_q[:, 1]], axis=1)
    partner = jnp.where(lax.axis_index("seq") == 0, own_pair, reversed_q[:, ::-1])
    first = jnp.stack([0.5 * (packed[0] + partner[0]), 0.5 * (packed[1] - partner[1])])
    second = jnp.stack([0.5 * (packed[1] + partner[1]), 0.5 * (partner[0] - packed[0])])
    return (first, second)


def inverse_rows(spectra):
    seq_count = lax.axis_size("seq")
    row_count = spectra.shape[2]
    period_len = 2 * row_count * seq_count
    inner_table = angle_table(row_count, row_count, row_count)
    cos_inner = jnp.cos(inner_table)
    sin_inner = jnp.sin(inner_table)
    real_sum = contract("qr,krw->kqw", cos_inner, spectra[0]) - contract(
        "qr,krw->kqw", sin_inner, spectra[1]
    )
    imag_sum = contract("qr,krw->kqw", cos_inner, spectra[1]) + contract(
        "qr,krw->kqw", sin_inner, spectra[0]
    )
    coarse = coarse_order(
        2 * lax.axis_index("seq") + lax.broadcasted_iota(jnp.int32, (2, row_count), 0), seq_count
    )
    position = lax.broadcasted_iota(jnp.int32, (2, row_count), 1)
    phases = angle_of(position * coarse, period_len)
    cos_turn = jnp.cos(phases)[:, :, None]
    sin_turn = jnp.sin(phases)[:, :, None]
    rotated = jnp.stack(
        [real_sum * cos_turn - imag_sum * sin_turn, real_sum * sin_turn + imag_sum * cos_turn]
    )
    target_grid = lax.broadcasted_iota(jnp.int32, (seq_count, 2 * seq_count), 0)
    slot_grid = lax.broadcasted_iota(jnp.int32, (seq_count, 2 * seq_count), 1)
    last_table = angle_of(target_grid * coarse_order(slot_grid, seq_count), 2 * seq_count)
    cos_last = jnp.cos(last_table)
    sin_last = jnp.sin(last_table)
    pieces = lax.all_to_all(rotated, "seq", split_axis=2, concat_axis=1, tiled=True)
    value = contract("sk,krw->srw", cos_last, pieces[0]) - contract(
        "sk,krw->srw", sin_last, pieces[1]
    )
    other = contract("sk,krw->srw", sin_last, pieces[0]) + contract(
        "sk,krw->srw", cos_last, pieces[1]
    )
    gathered = (value / period_len, other / period_len)
    gathered = jnp.concatenate([gathered[0], gathered[1]], axis=2)
    home_rows = lax.all_to_all(gathered, "seq", split_axis=0, concat_axis=1, tiled=True)
    return home_rows.reshape(row_count, home_rows.shape[2])


def invert_all(spectra):
    half_width = spectra.shape[3] // 2
    joined = jnp.stack(
        [
            spectra[0, :, :, :half_width] - spectra[1, :, :, half_width:],
            spectra[1, :, :, :half_width] + spectra[0, :, :, half_width:],
        ]
    )
    return inverse_rows(joined)


def shards(signal, grad_out, filter_taps, skip_gain):
    channels = filter_taps.shape[1]
    signal_rows = signal[0].astype(jnp.float32)
    grad_rows = grad_out[0].astype(jnp.float32)
    tap_half = filter_taps.shape[1] // 2
    columns = jnp.concatenate(
        [signal_rows, filter_taps[:, :tap_half], grad_rows, filter_taps[:, tap_half:]], axis=1
    )
    first, second = split_pairs(forward_spectra(columns))
    signal_spec = first[:, :, :, :channels]
    grad_spec = second[:, :, :, :channels]
    own_spec = jnp.concatenate([first[:, :, :, channels:], second[:, :, :, channels:]], axis=3)
    input_spec = jnp.stack(
        [
            grad_spec[0] * own_spec[0] + grad_spec[1] * own_spec[1],
            grad_spec[1] * own_spec[0] - grad_spec[0] * own_spec[1],
        ]
    )
    filter_terms = jnp.stack(
        [
            grad_spec[0] * signal_spec[0] + grad_spec[1] * signal_spec[1],
            grad_spec[1] * signal_spec[0] - grad_spec[0] * signal_spec[1],
        ]
    )
    summed = lax.psum(filter_terms, "batch")
    rows_back = invert_all(jnp.concatenate([input_spec, summed], axis=3))
    filter_grad = rows_back[:, channels:]
    input_grad = (rows_back[:, :channels] + skip_gain[None, :] * grad_rows).astype(jnp.bfloat16)
    return (input_grad[None], filter_grad)


def solution(mesh):
    groups, seqs = mesh.shape["batch"], mesh.shape["seq"]

    def either(signal, grad_out, filter_taps, skip_gain):
        if fits_fused(groups, seqs, signal, filter_taps):
            return fused_shards(groups, seqs, signal, grad_out, filter_taps, skip_gain)
        return shards(signal, grad_out, filter_taps, skip_gain)

    return jax.shard_map(
        either,
        mesh=mesh,
        in_specs=(P("batch", "seq", None), P("batch", "seq", None), P("seq", None), P()),
        out_specs=(P("batch", "seq", None), P("seq", None)),
        check_vma=False,
    )
```

```python
import functools
import math

import jax
import jax.numpy as jnp
import numpy as np
from jax import lax
from jax.experimental import pallas as pl
from jax.experimental.pallas import tpu as pltpu
from jax.sharding import PartitionSpec as P

MESH = pl.DeviceIdType.MESH
F32 = jnp.float32
BF16 = jnp.bfloat16
GRAD, TAPS, SIGNAL, INPUT, FILTER, FORWARD = range(6)


def weighted(terms):
    total = None
    for factor, array in terms:
        if array is None or abs(factor) < 1e-12:
            continue
        if total is None:
            if abs(factor - 1.0) < 1e-12:
                total = array
            else:
                total = array * factor
        elif abs(factor - 1.0) < 1e-12:
            total = total + array
        elif abs(factor + 1.0) < 1e-12:
            total = total - array
        else:
            total = total + array * factor
    return total


def added(left, right):
    return weighted([(1.0, left), (1.0, right)])


def subtracted(left, right):
    return weighted([(1.0, left), (-1.0, right)])


def turn(real, imag, cos_turn, sin_turn):
    if imag is None:
        return real * cos_turn, -(real * sin_turn)
    return real * cos_turn + imag * sin_turn, imag * cos_turn - real * sin_turn


def coarse_forward(blocks):
    count = len(blocks)
    result = [None] * (count + 1)
    for k in range(count // 2 + 1):
        sums = []
        for parity in (0, 1):
            angles = [(math.pi * ((s * k) % (2 * count)) / count, s) for s in range(parity, count, 2)]
            sums.append(
                (
                    weighted([(math.cos(a), blocks[s]) for a, s in angles]),
                    weighted([(-math.sin(a), blocks[s]) for a, s in angles]),
                )
            )
        (even_re, even_im), (odd_re, odd_im) = sums
        result[k] = (added(even_re, odd_re), added(even_im, odd_im))
        if k != count - k:
            result[count - k] = (subtracted(even_re, odd_re), subtracted(odd_im, even_im))
    return result


def coarse_inverse(terms, scale):
    count = len(terms) - 1
    pairs = []
    for k in range(count // 2 + 1):
        weight = scale if k == 0 else 2.0 * scale
        real, imag = terms[k]
        if k == count - k:
            pairs.append((weight, real, imag, real, imag))
        else:
            other_re, other_im = terms[count - k]
            pairs.append((weight, real + other_re, imag - other_im, real - other_re, imag + other_im))
    blocks = []
    for s in range(count):
        parts = []
        for k, (weight, even_re, even_im, odd_re, odd_im) in enumerate(pairs):
            angle = math.pi * ((s * k) % (2 * count)) / count
            parts.append((weight * math.cos(angle) * (1 if abs(math.cos(angle)) > 1e-9 else 0), odd_re if s % 2 else even_re))
            parts.append((weight * math.sin(angle) * (1 if abs(math.sin(angle)) > 1e-9 else 0), odd_im if s % 2 else even_im))
        blocks.append(weighted(parts))
    return blocks


def fused_kernel(
    groups, seqs,
    signal_hbm, grad_hbm, tap_hbm, skip_hbm, high_hbm, low_hbm, cos_hbm, sin_hbm,
    input_ref, filter_ref,
    signal_ref, grad_ref, tap_ref, skip_ref, high_ref, low_ref, cos_ref, sin_ref,
    grad_out_buf, signal_out_buf, tap_out_buf, grad_in, signal_in, tap_in,
    input_out, filter_out, input_in, filter_in,
    tap_rows, tap_spec, grad_rows, grad_spec, signal_rows, signal_spec, input_rows, filter_rows, filter_spec,
    send_sems, recv_sems, load_sems,
):
    count = groups * seqs
    coarse = seqs + 1
    own, rows = grad_in.shape[1:]
    channels = count * own
    group, seq = lax.axis_index("batch"), lax.axis_index("seq")
    me = group * seqs + seq
    scale = 1.0 / (2 * seqs * rows)
    re, im = pl.ds(0, rows), pl.ds(rows, rows)

    parity, pair = lax.rem(group, 2), lax.div(group, 2)
    half_seqs, half_groups = seqs // 2, groups // 2
    upper, inner = lax.div(seq, half_seqs), lax.rem(seq, half_seqs)

    def load(index, source, target):
        return pltpu.make_async_copy(source, target, load_sems.at[index])

    loads = [
        load(index, source, target)
        for index, (source, target) in enumerate(
            (
                (grad_hbm, grad_ref), (tap_hbm, tap_ref), (signal_hbm, signal_ref),
                (cos_hbm, cos_ref), (sin_hbm, sin_ref), (high_hbm, high_ref),
                (low_hbm, low_ref), (skip_hbm, skip_ref),
            )
        )
    ]
    for copy in loads:
        copy.start()

    def seq_at(step):
        other = lax.rem(upper + 1 + lax.div(step, half_seqs), 2)
        return other * half_seqs + lax.rem(inner + step, half_seqs)

    def peer(step):
        to_seq = seq_at(lax.div(step, groups))
        to_group = lax.rem(group + step, groups)
        return to_group * seqs + to_seq, to_group, to_seq

    def over_peers(body, total, own_step):
        lax.fori_loop(0, own_step, body, 0)
        lax.fori_loop(own_step + 1, total, body, 0)

    barrier = pltpu.get_barrier_semaphore()

    def greet(step, carry):
        _, to_group, to_seq = peer(step)
        pl.semaphore_signal(
            barrier, inc=1, device_id={"batch": to_group, "seq": to_seq}, device_id_type=MESH
        )
        return carry

    over_peers(greet, count, half_seqs * groups)

    def transfer(source, target, kind, to_group, to_seq):
        return pltpu.make_async_remote_copy(
            src_ref=source,
            dst_ref=target,
            send_sem=send_sems.at[kind],
            recv_sem=recv_sems.at[kind],
            device_id={"batch": to_group, "seq": to_seq},
            device_id_type=MESH,
        )

    def all_of(buffer, blocks, kind):
        _, to_group, to_seq = peer(0)
        view = buffer.at[pl.ds(0, blocks)]
        return transfer(view, view, kind, to_group, to_seq)

    loads[GRAD].wait()
    grad_out_buf[...] = grad_ref[...].astype(F32).T.reshape(count, own, rows)
    loads[TAPS].wait()
    tap_out_buf[...] = tap_ref[...].T.reshape(count, own, rows)
    pl.semaphore_wait(barrier, count - 1)

    def send_taps(step, carry):
        to_seq = seq_at(step)
        place = group * seqs + to_seq
        transfer(tap_out_buf.at[place], tap_in.at[seq], TAPS, group, to_seq).start()
        return carry

    def send_grads(step, carry):
        place, to_group, to_seq = peer(step)
        transfer(grad_out_buf.at[place], grad_in.at[me], GRAD, to_group, to_seq).start()
        return carry

    def send_signals(step, carry):
        place, to_group, to_seq = peer(step)
        transfer(signal_out_buf.at[place], signal_in.at[me], SIGNAL, to_group, to_seq).start()
        return carry

    over_peers(send_taps, seqs, half_seqs)
    over_peers(send_grads, count, half_seqs * groups)
    loads[SIGNAL].wait()
    signal_out_buf[...] = signal_ref[...].astype(F32).T.reshape(count, own, rows)
    over_peers(send_signals, count, half_seqs * groups)
    grad_in[me] = grad_out_buf[me]
    tap_in[seq] = tap_out_buf[me]
    signal_in[me] = signal_out_buf[me]

    def spread(blocks, target, first_row):
        place = pl.ds(first_row, own)
        for k, (real, imag) in enumerate(coarse_forward(blocks)):
            real, imag = turn(real, imag, cos_ref[k], sin_ref[k])
            target[k, place, re] = real
            target[k, place, im] = imag

    def fine(source, target):
        lines = source.shape[0] * source.shape[1]
        value = source[...].reshape(lines, 2 * rows)
        high = value.astype(BF16)
        low = (value - high.astype(F32)).astype(BF16)
        product = functools.partial(jnp.dot, preferred_element_type=F32)
        total = product(high, high_ref[...]) + product(low, high_ref[...]) + product(high, low_ref[...])
        target[...] = total.reshape(target.shape)

    def collect(source, first_row):
        place = pl.ds(first_row, own)
        terms = [
            turn(source[k, place, re], source[k, place, im], cos_ref[k], sin_ref[k])
            for k in range(coarse)
        ]
        return coarse_inverse(terms, scale)

    def row_of(index):
        return pl.multiple_of(index * own, own)

    for copy in loads[3:]:
        copy.wait()
    all_of(tap_in, seqs - 1, TAPS).wait_recv()
    spread([tap_in[s] for s in range(seqs)], tap_rows, 0)
    fine(tap_rows, tap_spec)
    all_of(grad_in, count - 1, GRAD).wait_recv()

    def group_at(index):
        return lax.rem(2 * pair + index, groups)

    def input_part(first):
        source, spectrum, lines = grad_rows.at[first], grad_spec.at[first], input_rows.at[first]

        def spread_grad(index, carry):
            here = group_at(2 * first + index)
            spread([grad_in[here * seqs + s] for s in range(seqs)], source, row_of(index))
            return carry

        lax.fori_loop(0, 2, spread_grad, 0)
        fine(source, spectrum)

        def multiply_taps(index, carry):
            place = pl.ds(row_of(index), own)
            for k in range(coarse):
                grad_re, grad_im = spectrum[k, place, re], spectrum[k, place, im]
                tap_re, tap_im = tap_spec[k, :, re], tap_spec[k, :, im]
                lines[k, place, re] = grad_re * tap_re + grad_im * tap_im
                lines[k, place, im] = grad_re * tap_im - grad_im * tap_re
            return carry

        lax.fori_loop(0, 2, multiply_taps, 0)
        fine(lines, lines)

        def collect_input(index, carry):
            here = group_at(2 * first + index)
            for s, block in enumerate(collect(lines, row_of(index))):
                input_out[here * seqs + s] = block
            return carry

        lax.fori_loop(0, 2, collect_input, 0)

        def send_inputs(step, carry):
            to_seq = seq_at(lax.div(step, 2))
            to_group = group_at(2 * first + lax.rem(parity + step, 2))
            place = to_group * seqs + to_seq
            transfer(input_out.at[place], input_in.at[me], INPUT, to_group, to_seq).start()
            return carry

        if first == 0:
            over_peers(send_inputs, 2 * seqs, 2 * half_seqs)
        else:
            lax.fori_loop(0, 2 * seqs, send_inputs, 0)

    for first in reversed(range(half_groups)):
        input_part(first)
    input_in[me] = input_out[me]

    all_of(signal_in, count - 1, SIGNAL).wait_recv()

    def spread_signal(index, carry):
        here = group_at(index)
        spread([signal_in[here * seqs + s] for s in range(seqs)], signal_rows, row_of(index))
        return carry

    lax.fori_loop(0, groups, spread_signal, 0)
    fine(signal_rows, signal_spec)
    for k in range(coarse):
        real, imag = None, None
        for index in range(groups):
            place = pl.ds(index * own, own)
            which, local = index // 2, pl.ds(index % 2 * own, own)
            grad_re, grad_im = grad_spec[which, k, local, re], grad_spec[which, k, local, im]
            signal_re, signal_im = signal_spec[k, place, re], signal_spec[k, place, im]
            real = added(real, grad_re * signal_re + grad_im * signal_im)
            imag = added(imag, grad_re * signal_im - grad_im * signal_re)
        filter_rows[k, :, re] = real
        filter_rows[k, :, im] = imag
    fine(filter_rows, filter_spec)
    for s, block in enumerate(collect(filter_spec, 0)):
        filter_out[s] = block

    def send_filters(step, carry):
        to_seq = seq_at(lax.div(step, half_groups))
        to_group = 2 * lax.rem(pair + step, half_groups) + parity
        place = pair * seqs + seq
        transfer(
            filter_out.at[to_seq], filter_in.at[parity, place], FILTER, to_group, to_seq
        ).start()
        return carry

    over_peers(send_filters, seqs * half_groups, half_seqs * half_groups)
    filter_in[parity, pair * seqs + seq] = filter_out[seq]

    half = count // 2
    all_of(input_in, count - 1, INPUT).wait_recv()
    gradient = input_in[...].reshape(channels, rows).T + skip_ref[...] * grad_ref[...].astype(F32)
    input_ref[...] = gradient.astype(BF16)
    all_of(filter_in.at[0], half - 1, FILTER).wait_recv()
    mine = filter_in.at[parity]
    partner = 2 * pair + 1 - parity
    forward = transfer(mine, mine, FORWARD, partner, seq)
    forward.start()
    forward.wait_recv()
    parts = [
        filter_in[which, first * seqs : (first + 1) * seqs].reshape(seqs * own, rows)
        for first in range(half_groups)
        for which in range(2)
    ]
    filter_ref[...] = jnp.concatenate(parts, axis=0).T
    for kind, buffer in ((GRAD, grad_in), (SIGNAL, signal_in), (INPUT, input_in)):
        all_of(buffer, count - 1, kind).wait_send()
    all_of(filter_in.at[0], half - 1, FILTER).wait_send()
    forward.wait_send()
    all_of(tap_in, seqs - 1, TAPS).wait_send()


def fine_tables(rows):
    grid = np.arange(rows)
    angle = 2.0 * np.pi / rows * (np.outer(grid, grid) % rows)
    table = np.block([[np.cos(angle), -np.sin(angle)], [np.sin(angle), np.cos(angle)]]).astype(np.float32)
    high = table.astype(BF16)
    return high, (table - high.astype(np.float32)).astype(BF16)


def turn_tables(seqs, rows, lines):
    angle = np.pi / (seqs * rows) * np.outer(np.arange(seqs + 1), np.arange(rows))
    wide = np.broadcast_to(angle[:, None, :], (seqs + 1, lines, rows))
    return np.cos(wide).astype(np.float32), np.sin(wide).astype(np.float32)


def fused_shards(groups, seqs, signal, grad_out, filter_taps, skip_gain):
    rows, channels = filter_taps.shape
    count, coarse = groups * seqs, seqs + 1
    own = channels // count
    high, low = fine_tables(rows)
    cos_turn, sin_turn = turn_tables(seqs, rows, own)
    blocks = pltpu.VMEM((count, own, rows), F32)
    few = pltpu.VMEM((seqs, own, rows), F32)
    lines = lambda number: pltpu.VMEM((coarse, number * own, 2 * rows), F32)
    pairs = pltpu.VMEM((groups // 2, coarse, 2 * own, 2 * rows), F32)
    vmem = pl.BlockSpec(memory_space=pltpu.VMEM)
    hbm = pl.BlockSpec(memory_space=pltpu.HBM)
    turns = pltpu.VMEM((coarse, own, rows), F32)
    table = pltpu.VMEM((2 * rows, 2 * rows), BF16)
    input_grad, filter_grad = pl.pallas_call(
        functools.partial(fused_kernel, groups, seqs),
        out_shape=(
            jax.ShapeDtypeStruct((rows, channels), BF16),
            jax.ShapeDtypeStruct((rows, channels), F32),
        ),
        in_specs=[hbm] * 8,
        out_specs=(vmem, vmem),
        scratch_shapes=[
            pltpu.VMEM((rows, channels), BF16), pltpu.VMEM((rows, channels), BF16),
            pltpu.VMEM((rows, channels), F32), pltpu.VMEM((1, channels), F32),
            table, table, turns, turns,
            blocks, blocks, blocks, blocks, blocks, few,
            blocks, few, blocks, pltpu.VMEM((2, count // 2, own, rows), F32),
            lines(1), lines(1), pairs, pairs, lines(groups), lines(groups),
            pairs, lines(1), lines(1),
            pltpu.SemaphoreType.DMA((6,)),
            pltpu.SemaphoreType.DMA((6,)),
            pltpu.SemaphoreType.DMA((8,)),
        ],
        compiler_params=pltpu.CompilerParams(
            collective_id=0, has_side_effects=True, vmem_limit_bytes=67_043_328
        ),
    )(
        signal[0], grad_out[0], filter_taps, skip_gain[None, :],
        jnp.asarray(high), jnp.asarray(low), jnp.asarray(cos_turn), jnp.asarray(sin_turn),
    )
    return input_grad[None], filter_grad


def fits_fused(groups, seqs, signal, filter_taps):
    rows, channels = filter_taps.shape
    return (
        signal.shape[0] == 1
        and seqs % 2 == 0
        and groups % 2 == 0
        and rows % 128 == 0
        and channels % (8 * groups * seqs) == 0
    )


def angle_table(height, width, period):
    product = lax.broadcasted_iota(jnp.int32, (height, width), 0) * lax.broadcasted_iota(
        jnp.int32, (height, width), 1
    )
    return 2.0 * jnp.pi / period * (product % period).astype(jnp.float32)


def angle_of(product, period):
    return 2.0 * jnp.pi / period * (product % period).astype(jnp.float32)


def coarse_order(slot, seq_count):
    pair_index = slot // 2
    odd_slot = slot % 2
    return jnp.where(
        pair_index == 0,
        odd_slot * seq_count,
        jnp.where(odd_slot == 0, pair_index, 2 * seq_count - pair_index),
    )


def contract(form, table, operand):
    return jnp.einsum(form, table, operand, precision=lax.Precision.HIGHEST)


def forward_spectra(columns):
    seq_count = lax.axis_size("seq")
    row_count = columns.shape[0]
    part_rows = row_count // seq_count
    period_len = 2 * row_count * seq_count
    spread = lax.all_to_all(
        columns.reshape(1, row_count, columns.shape[1]),
        "seq",
        split_axis=1,
        concat_axis=0,
        tiled=True,
    )
    slot_grid = lax.broadcasted_iota(jnp.int32, (2 * seq_count, seq_count), 0)
    source_grid = lax.broadcasted_iota(jnp.int32, (2 * seq_count, seq_count), 1)
    first_table = angle_of(coarse_order(slot_grid, seq_count) * source_grid, 2 * seq_count)
    cos_first = jnp.cos(first_table)
    sin_first = jnp.sin(first_table)
    half_width = spread.shape[2] // 2
    real_in = spread[:, :, :half_width]
    imag_in = spread[:, :, half_width:]
    real_part = contract("ks,srw->krw", cos_first, real_in) + contract(
        "ks,srw->krw", sin_first, imag_in
    )
    imag_part = contract("ks,srw->krw", cos_first, imag_in) - contract(
        "ks,srw->krw", sin_first, real_in
    )
    global_row = lax.axis_index("seq") * part_rows + lax.broadcasted_iota(
        jnp.int32, (2 * seq_count, part_rows), 1
    )
    coarse = coarse_order(lax.broadcasted_iota(jnp.int32, (2 * seq_count, part_rows), 0), seq_count)
    phases = angle_of(global_row * coarse, period_len)
    cos_turn = jnp.cos(phases)[:, :, None]
    sin_turn = jnp.sin(phases)[:, :, None]
    rotated = jnp.stack(
        [real_part * cos_turn + imag_part * sin_turn, imag_part * cos_turn - real_part * sin_turn]
    )
    inner_table = angle_table(row_count, row_count, row_count)
    cos_inner = jnp.cos(inner_table)
    sin_inner = jnp.sin(inner_table)
    pieces = lax.all_to_all(rotated, "seq", split_axis=1, concat_axis=2, tiled=True)
    real_sum = contract("qr,krw->kqw", cos_inner, pieces[0]) + contract(
        "qr,krw->kqw", sin_inner, pieces[1]
    )
    imag_sum = contract("qr,krw->kqw", cos_inner, pieces[1]) - contract(
        "qr,krw->kqw", sin_inner, pieces[0]
    )
    return jnp.stack([real_sum, imag_sum])


def split_pairs(packed):
    reversed_q = packed[:, :, ::-1]
    zero_row = jnp.roll(reversed_q[:, 0], 1, axis=1)
    own_pair = jnp.stack([zero_row, reversed_q[:, 1]], axis=1)
    partner = jnp.where(lax.axis_index("seq") == 0, own_pair, reversed_q[:, ::-1])
    first = jnp.stack([0.5 * (packed[0] + partner[0]), 0.5 * (packed[1] - partner[1])])
    second = jnp.stack([0.5 * (packed[1] + partner[1]), 0.5 * (partner[0] - packed[0])])
    return (first, second)


def inverse_rows(spectra):
    seq_count = lax.axis_size("seq")
    row_count = spectra.shape[2]
    period_len = 2 * row_count * seq_count
    inner_table = angle_table(row_count, row_count, row_count)
    cos_inner = jnp.cos(inner_table)
    sin_inner = jnp.sin(inner_table)
    real_sum = contract("qr,krw->kqw", cos_inner, spectra[0]) - contract(
        "qr,krw->kqw", sin_inner, spectra[1]
    )
    imag_sum = contract("qr,krw->kqw", cos_inner, spectra[1]) + contract(
        "qr,krw->kqw", sin_inner, spectra[0]
    )
    coarse = coarse_order(
        2 * lax.axis_index("seq") + lax.broadcasted_iota(jnp.int32, (2, row_count), 0), seq_count
    )
    position = lax.broadcasted_iota(jnp.int32, (2, row_count), 1)
    phases = angle_of(position * coarse, period_len)
    cos_turn = jnp.cos(phases)[:, :, None]
    sin_turn = jnp.sin(phases)[:, :, None]
    rotated = jnp.stack(
        [real_sum * cos_turn - imag_sum * sin_turn, real_sum * sin_turn + imag_sum * cos_turn]
    )
    target_grid = lax.broadcasted_iota(jnp.int32, (seq_count, 2 * seq_count), 0)
    slot_grid = lax.broadcasted_iota(jnp.int32, (seq_count, 2 * seq_count), 1)
    last_table = angle_of(target_grid * coarse_order(slot_grid, seq_count), 2 * seq_count)
    cos_last = jnp.cos(last_table)
    sin_last = jnp.sin(last_table)
    pieces = lax.all_to_all(rotated, "seq", split_axis=2, concat_axis=1, tiled=True)
    value = contract("sk,krw->srw", cos_last, pieces[0]) - contract(
        "sk,krw->srw", sin_last, pieces[1]
    )
    other = contract("sk,krw->srw", sin_last, pieces[0]) + contract(
        "sk,krw->srw", cos_last, pieces[1]
    )
    gathered = (value / period_len, other / period_len)
    gathered = jnp.concatenate([gathered[0], gathered[1]], axis=2)
    home_rows = lax.all_to_all(gathered, "seq", split_axis=0, concat_axis=1, tiled=True)
    return home_rows.reshape(row_count, home_rows.shape[2])


def invert_all(spectra):
    half_width = spectra.shape[3] // 2
    joined = jnp.stack(
        [
            spectra[0, :, :, :half_width] - spectra[1, :, :, half_width:],
            spectra[1, :, :, :half_width] + spectra[0, :, :, half_width:],
        ]
    )
    return inverse_rows(joined)


def shards(signal, grad_out, filter_taps, skip_gain):
    channels = filter_taps.shape[1]
    signal_rows = signal[0].astype(jnp.float32)
    grad_rows = grad_out[0].astype(jnp.float32)
    tap_half = filter_taps.shape[1] // 2
    columns = jnp.concatenate(
        [signal_rows, filter_taps[:, :tap_half], grad_rows, filter_taps[:, tap_half:]], axis=1
    )
    first, second = split_pairs(forward_spectra(columns))
    signal_spec = first[:, :, :, :channels]
    grad_spec = second[:, :, :, :channels]
    own_spec = jnp.concatenate([first[:, :, :, channels:], second[:, :, :, channels:]], axis=3)
    input_spec = jnp.stack(
        [
            grad_spec[0] * own_spec[0] + grad_spec[1] * own_spec[1],
            grad_spec[1] * own_spec[0] - grad_spec[0] * own_spec[1],
        ]
    )
    filter_terms = jnp.stack(
        [
            grad_spec[0] * signal_spec[0] + grad_spec[1] * signal_spec[1],
            grad_spec[1] * signal_spec[0] - grad_spec[0] * signal_spec[1],
        ]
    )
    summed = lax.psum(filter_terms, "batch")
    rows_back = invert_all(jnp.concatenate([input_spec, summed], axis=3))
    filter_grad = rows_back[:, channels:]
    input_grad = (rows_back[:, :channels] + skip_gain[None, :] * grad_rows).astype(jnp.bfloat16)
    return (input_grad[None], filter_grad)


def solution(mesh):
    groups, seqs = mesh.shape["batch"], mesh.shape["seq"]

    def either(signal, grad_out, filter_taps, skip_gain):
        if fits_fused(groups, seqs, signal, filter_taps):
            return fused_shards(groups, seqs, signal, grad_out, filter_taps, skip_gain)
        return shards(signal, grad_out, filter_taps, skip_gain)

    return jax.shard_map(
        either,
        mesh=mesh,
        in_specs=(P("batch", "seq", None), P("batch", "seq", None), P("seq", None), P()),
        out_specs=(P("batch", "seq", None), P("seq", None)),
        check_vma=False,
    )
```
